32 devices in a mesh: pipe: 2 (over x), dp: 4 (over z), tensor: 4 (over y, core).
Axes of the slice: x: 2, y: 2, z: 4, core: 2. Of those that a mesh axis runs over, the one named last changes fastest.
Arguments:
- acts_in: bfloat16 [2, 512, 4096], P(None, 'dp', 'tensor'), may hold values from -6 to 6
- weights: bfloat16 [2, 4096, 4096], P('pipe', None, 'tensor'), may hold values from -0.046875 to 0.046875
- cotangent: bfloat16 [2, 512, 4096], P(None, 'dp', 'tensor'), may hold values from -6 to 6
- hist_act: float32 [2, 16], P('pipe'), may hold values from 2 to 12
- hist_weight: float32 [2, 16], P('pipe'), may hold values from 0.01 to 0.1
- hist_grad: float32 [2, 16], P('pipe'), may hold values from 2 to 12
Outputs:
- section_acts: bfloat16 [2, 2, 512, 4096], P('pipe', None, 'dp', 'tensor')
- section_grads: bfloat16 [2, 2, 512, 4096], P('pipe', None, 'dp', 'tensor')
- weight_grad: bfloat16 [2, 4096, 4096], P('pipe', 'dp', 'tensor')
- new_hist_act: float32 [2, 16], P('pipe')
- new_hist_weight: float32 [2, 16], P('pipe')
- new_hist_grad: float32 [2, 16], P('pipe')
The draws below stay inside these ranges and needn't reach their ends.
All inputs are finite; a program needn't handle non-finite values.
Results may differ from the reference program's by a relative error of at most 0.025.
Values may be sent and summed in bfloat16 or wider, within the bound.
A program may use at most 128 MiB of HBM per device.

```python
import math
import jax
import jax.numpy as jnp
from jax import lax

D = 4096
ROWS = 128
MICRO = 2
HIST = 16
SECTIONS = 2
BATCH = 512
N_DP = 4
N_TENSOR = 4


def steps_of(key, dims, split, least, high):
    factor_of, own = 1.0, jax.random.fold_in(key, 6)
    for axis_at, blocks in split:
        draws = jnp.exp(jax.random.uniform(jax.random.fold_in(own, axis_at), (blocks,), jnp.float32, least / len(split), high / len(split)))
        factor_of = factor_of * jnp.repeat(draws, dims[axis_at] // blocks).reshape([-1 if axis == axis_at else 1 for axis in range(len(dims))])
    return factor_of


def centred(rng, shape, scale, reach, pieces=(), kind=jnp.bfloat16):
    factor_of = steps_of(rng, shape, pieces, -0.22, 0.18) if pieces else 1.0
    result = jax.random.normal(rng, shape, jnp.float32) * scale * factor_of
    return jnp.minimum(jnp.maximum(result, -reach), reach).astype(kind)


def setup_inputs(seed: int = 0) -> dict:
    seeds = jax.random.split(jax.random.key(seed), 7)
    acts_in = centred(seeds[0], (MICRO, BATCH, D), 1.0, 6.0, ((1, 4), (2, 4)))
    weights = centred(seeds[1], (SECTIONS, D, D), (4 * D) ** -0.5, 0.046875, ((0, 2), (2, 4)))
    cotangent = centred(seeds[2], (MICRO, BATCH, D), 1.0, 6.0, ((1, 4), (2, 4)))
    hist_act = jnp.clip(jnp.exp(math.log(12.0) - 1.7917595 * jax.random.uniform(seeds[3], (SECTIONS, HIST), jnp.float32) ** steps_of(seeds[3], (SECTIONS, HIST), ((0, 2),), -0.2, 0.2)), 2.0, 12.0)
    hist_weight = jnp.clip(jnp.exp(math.log(0.1) - 2.3025851 * jax.random.uniform(seeds[4], (SECTIONS, HIST), jnp.float32) ** steps_of(seeds[4], (SECTIONS, HIST), ((0, 2),), -0.2, 0.2)), 0.01, 0.1)
    hist_grad = jnp.clip(jnp.exp(math.log(12.0) - 1.7917595 * jax.random.uniform(seeds[5], (SECTIONS, HIST), jnp.float32) ** steps_of(seeds[5], (SECTIONS, HIST), ((0, 2),), -0.2, 0.2)), 2.0, 12.0)
    return {"acts_in": acts_in, "weights": weights, "cotangent": cotangent, "hist_act": hist_act, "hist_weight": hist_weight, "hist_grad": hist_grad}


def quantize(values, factor, limit_value):
    return jnp.clip(values.astype(jnp.float32) * factor, -limit_value, limit_value).astype(jnp.bfloat16)


def settle(values):
    return lax.optimization_barrier(values.astype(jnp.bfloat16)).astype(jnp.float32)


def roll_history(history, newest):
    return jnp.concatenate([newest[:, None], history[:, :-1]], axis=1)


def reference(acts_in, weights, cotangent, hist_act, hist_weight, hist_grad):
    section_count = weights.shape[0]
    full_width = weights.shape[1]
    block_width = full_width // N_TENSOR
    current = acts_in.reshape(-1, full_width)
    act_factors = []
    weight_factors = []
    quant_acts = []
    quant_weights = []
    outputs = []
    act_peaks = []
    weight_peaks = []
    for section_index in range(section_count):
        act_factor = 448.0 / jnp.max(hist_act[section_index])
        weight_factor = 448.0 / jnp.max(hist_weight[section_index])
        quant_weight = quantize(weights[section_index], weight_factor, 448.0)
        quant_act = quantize(current, act_factor, 448.0)
        act_peaks.append(jnp.max(jnp.abs(current.astype(jnp.float32))))
        weight_peaks.append(jnp.max(jnp.abs(weights[section_index].astype(jnp.float32))))
        mixed_terms = jnp.dot(quant_act, quant_weight, preferred_element_type=jnp.float32) * (1.0 / (act_factor * weight_factor))
        current = (current.astype(jnp.float32) + mixed_terms).astype(jnp.bfloat16)
        outputs.append(current.reshape(MICRO, -1, full_width))
        act_factors.append(act_factor)
        weight_factors.append(weight_factor)
        quant_acts.append(quant_act)
        quant_weights.append(quant_weight)
    gradient = (cotangent.reshape(-1, full_width).astype(jnp.float32) * current.astype(jnp.float32)).astype(jnp.bfloat16)
    grads_out = [None] * section_count
    weight_sums = [None] * section_count
    grad_peaks = [None] * section_count
    for section_index in reversed(range(section_count)):
        grad_factor = 57344.0 / jnp.max(hist_grad[section_index])
        grad_peaks[section_index] = jnp.max(jnp.abs(gradient.astype(jnp.float32)))
        quant_grad = quantize(gradient, grad_factor, 57344.0)
        backward_factor = 1.0 / (grad_factor * weight_factors[section_index])
        sum_total = jnp.zeros((gradient.shape[0], full_width), jnp.float32)
        for shard_part in range(N_TENSOR):
            column_span = slice(shard_part * block_width, (shard_part + 1) * block_width)
            product_term = jnp.dot(quant_grad[:, column_span], quant_weights[section_index][:, column_span].T, preferred_element_type=jnp.float32) * backward_factor
            sum_total = sum_total + settle(product_term)
        gradient = (gradient.astype(jnp.float32) + sum_total).astype(jnp.bfloat16)
        grads_out[section_index] = gradient.reshape(MICRO, -1, full_width)
        update_factor = 1.0 / (act_factors[section_index] * grad_factor)
        acts_split = quant_acts[section_index].reshape(MICRO, N_DP, ROWS, full_width)
        grads_split = quant_grad.reshape(MICRO, N_DP, ROWS, full_width)
        weight_sum = jnp.zeros((full_width, full_width), jnp.float32)
        for dp_rank in range(N_DP):
            left_rows = acts_split[:, dp_rank].reshape(-1, full_width)
            right_rows = grads_split[:, dp_rank].reshape(-1, full_width)
            weight_sum = weight_sum + settle(jnp.dot(left_rows.T, right_rows, preferred_element_type=jnp.float32) * update_factor)
        weight_sums[section_index] = weight_sum.astype(jnp.bfloat16)
    section_acts = jnp.stack(outputs)
    section_grads = jnp.stack(grads_out)
    weight_grad = jnp.stack(weight_sums)
    new_hist_act = roll_history(hist_act, jnp.stack(act_peaks))
    new_hist_weight = roll_history(hist_weight, jnp.stack(weight_peaks))
    new_hist_grad = roll_history(hist_grad, jnp.stack(grad_peaks))
    return (section_acts, section_grads, weight_grad, new_hist_act, new_hist_weight, new_hist_grad)
```

```python
import functools

import jax
import jax.numpy as jnp
from jax import lax
from jax.experimental import pallas as pl
from jax.experimental.pallas import tpu as pltpu
from jax.sharding import PartitionSpec as P

MESH = pl.DeviceIdType.MESH
FIRST, LATER = (4, 4, 2), (2, 2)


def strides_below(index, count):
    low = (index & -index) if index else count
    step, found = low // 2, []
    while step:
        found.append(step)
        step //= 2
    return found


def low(i):
    return i & -i


def chunks_of(M, R):
    found = []
    for m in range(M):
        start = 0
        for part in FIRST if m == 0 else LATER:
            found.append((m, start, R // part))
            start += R // part
    return found


def kernel(S, N, T, M, R, F, FA, chunks,
           acts, weights, cot, hist_a, hist_w, hist_g,
           xout, gout, G, At, dw, out_top,
           w, wt, hv, cv, xin, xg, acc, gin, part, rs, A, pk, amax, gmax,
           w_sem, h_sem, in_sem, c_sem, x_ss, x_rs, ag_ss, ag_rs, g_ss, g_rs, rd_ss, rd_rs,
           G_ss, G_rs, Gr_ss, A_ss, A_rs, B_ss, B_rs, p_ss, p_rs, hello):
    s, d, t = lax.axis_index("pipe"), lax.axis_index("dp"), lax.axis_index("tensor")
    last = S - 1
    bf, f32 = jnp.bfloat16, jnp.float32
    NC = len(chunks)
    stages = []
    st = 1
    while st < T:
        stages.append(st)
        st *= 2

    def remote(src, dst, ss, rsem, **where):
        return pltpu.make_async_remote_copy(
            src_ref=src, dst_ref=dst, send_sem=ss, recv_sem=rsem,
            device_id=where, device_id_type=MESH)

    def signal(sem, **where):
        pl.semaphore_signal(sem, inc=1, device_id=where, device_id_type=MESH)

    barrier = pltpu.get_barrier_semaphore()
    for st in stages:
        signal(barrier, tensor=t ^ st)

    @pl.when(s > 0)
    def _():
        signal(barrier, pipe=s - 1)

    @pl.when(s < last)
    def _():
        signal(barrier, pipe=s + 1)

    @pl.when(d > 0)
    def _():
        signal(barrier, dp=d - 1)

    @pl.when(d < N - 1)
    def _():
        signal(barrier, dp=d + 1)

    def rows_at(c):
        m, start, n = chunks[c]
        return pl.ds(m * R + start, n)

    h_loads = [pltpu.make_async_copy(h, hv.at[i], h_sem)
               for i, h in enumerate((hist_a, hist_w, hist_g))]
    loads = [pltpu.make_async_copy(weights.at[b], w.at[b], w_sem.at[b]) for b in range(T)]
    first = chunks[0][2]
    in_loads = [pltpu.make_async_copy(acts.at[rows], xin.at[rows], in_sem.at[i])
                for i, rows in enumerate((pl.ds(0, first), pl.ds(first, M * R - first)))]
    cot_load = pltpu.make_async_copy(cot, cv, c_sem)
    for copy in h_loads:
        copy.start()

    @pl.when(s == 0)
    def _():
        for copy in in_loads:
            copy.start()

    pltpu.make_async_copy(hv, hv, h_sem).wait()
    for copy in loads:
        copy.start()

    @pl.when(s == last)
    def _():
        cot_load.start()

    def limit(i):
        return jnp.max(hv[i], axis=1, keepdims=True).astype(bf)

    lim_a, lim_w, lim_g = limit(0), limit(1), limit(2)

    def clip(v, lim):
        return jnp.minimum(jnp.maximum(v, -lim), lim)

    def fold(v):
        return jnp.max(jnp.abs(v).reshape(-1, 16, v.shape[-1]), axis=0)

    amax[...] = jnp.zeros_like(amax)
    gmax[...] = jnp.zeros_like(gmax)

    def enter():
        near = (s > 0).astype(jnp.int32) + (s < last).astype(jnp.int32)
        beside = (d > 0).astype(jnp.int32) + (d < N - 1).astype(jnp.int32)
        pl.semaphore_wait(barrier, len(stages) + near + beside)

    def greet(r):
        @pl.when(d > 0)
        def _():
            signal(hello.at[r, 0], dp=d - 1)

        @pl.when(d < N - 1)
        def _():
            signal(hello.at[r, 1], dp=d + 1)

    def greeted(r):
        @pl.when(d < N - 1)
        def _():
            pl.semaphore_wait(hello.at[r, 0], 1)

        @pl.when(d > 0)
        def _():
            pl.semaphore_wait(hello.at[r, 1], 1)

    up = jnp.minimum(s + 1, last)
    down = jnp.maximum(s - 1, 0)

    def x_copy(c):
        return remote(xout.at[rows_at(c)], xin.at[rows_at(c)], x_ss, x_rs.at[c], pipe=up)

    def g_copy(c):
        return remote(gout.at[rows_at(c)], gin.at[rows_at(c)], g_ss, g_rs.at[c], pipe=down)

    def ag_copy(c, j, st):
        i = j ^ st
        return remote(xg.at[j, rows_at(c)], xg.at[i, rows_at(c)], ag_ss, ag_rs.at[c, i - 1], tensor=t ^ st)

    def G_copy(c, origin, to, ss):
        m, start, n = chunks[c]
        rows = pl.ds(start, n)
        return remote(G.at[m, origin ^ d, rows], G.at[m, origin ^ to, rows], ss, G_rs.at[c, (origin ^ to) - 1], dp=to)

    def G_wait(c, origin):
        m, start, n = chunks[c]
        here = G.at[m, origin ^ d, pl.ds(start, n)]
        remote(here, here, G_ss.at[0], G_rs.at[c, (origin ^ d) - 1], dp=origin).wait_recv()

    def inside(at):
        return (at >= 0) & (at < N)

    def own_sends(act):
        for i, step in enumerate((1, -1, 2, -2)):
            if abs(step) < N:
                @pl.when(inside(d + step))
                def _(i=i, to=d + step):
                    act(to, G_ss.at[i])

    def relays(wait, act):
        for i, way in enumerate((1, -1)):
            for m in range(1, (N + 1) // 2):
                origin = d - way * 2 * m

                @pl.when(inside(origin) & inside(d + way))
                def _(i=i, way=way, m=m, origin=origin):
                    wait(origin)
                    for step in (1, 2):
                        if 2 * m + step < N:
                            @pl.when(inside(d + way * step))
                            def _(step=step):
                                act(origin, d + way * step, Gr_ss.at[i, m - 1, step - 1])

    ratio = N // T

    def in_block(r):
        start = lax.rem(r, ratio) * FA
        return t ^ lax.div(r, ratio), pl.ds(pl.multiple_of(start, FA), FA)

    piece = R // T

    def rows_of(owner):
        return pl.ds(pl.multiple_of(owner * piece, piece), piece)

    def A_copy(m, k):
        owner, cols = in_block(d ^ k)
        src = pl.ds(pl.multiple_of(m * R + t * piece, piece), piece)
        return remote(xg.at[owner, src, cols], A.at[m, k, rows_of(t)],
                      A_ss, A_rs.at[m], dp=d ^ k)

    def B_copy(m, j, st):
        i = j ^ st
        there = A.at[m, pl.ds(1, N - 1), rows_of(t ^ j)]
        return remote(there, there, B_ss, B_rs.at[m, i - 1], tensor=t ^ st)

    def B_arrival(m, i):
        there = A.at[m, pl.ds(1, N - 1), rows_of(t ^ i)]
        return remote(there, there, B_ss, B_rs.at[m, i - 1], tensor=t ^ low(i))

    def rd_copy(c, j, level):
        st = stages[level]
        i = j ^ st
        return remote(part.at[j, rows_at(c)], rs.at[level, i, rows_at(c)], rd_ss, rd_rs.at[c, i + st - 1],
                      tensor=t ^ st)

    def prep(c):
        rows = rows_at(c)

        @pl.when(s == 0)
        def _():
            if c < len(in_loads):
                in_loads[c].wait()

        @pl.when(s > 0)
        def _():
            x_copy(c).wait_recv()

        x = xin[rows]
        xg[0, rows] = clip(x, lim_a)
        for st in strides_below(0, T):
            ag_copy(c, 0, st).start()
        amax[...] = jnp.maximum(amax[...], fold(x))

    def clip_weights():
        peak = jnp.zeros((16, F), bf)
        for b in range(T):
            loads[b].wait()

            def body(i, m, b=b):
                rows = pl.ds(pl.multiple_of(i * 128, 128), 128)
                v = w[b, rows]
                w[b, rows] = clip(v, lim_w)
                return jnp.maximum(m, fold(v))

            peak = lax.fori_loop(0, F // 128, body, peak)
        return jnp.max(peak.astype(f32), keepdims=True).reshape(1, 1)

    def turn_weights():
        for b in range(T):
            def body(i, _, b=b):
                rows = pl.ds(pl.multiple_of(i * 128, 128), 128)
                wt[b, :, rows] = w[b, rows].T
                return 0

            lax.fori_loop(0, F // 128, body, 0)

    def fwd(c):
        rows = rows_at(c)
        n = chunks[c][2]

        def term(j):
            return jnp.dot(xg[j, rows], w[t ^ j], preferred_element_type=f32)

        for j in range(T):
            if j:
                ag_copy(c, j ^ low(j), low(j)).wait_recv()
                for st in strides_below(j, T):
                    ag_copy(c, j, st).start()
            if j == 0:
                if T == 1:
                    xout[rows] = (term(0) + xin[rows].astype(f32)).astype(bf)
            elif j == 1:
                y = term(0) + term(1)
                if T == 2:
                    xout[rows] = (y + xin[rows].astype(f32)).astype(bf)
                else:
                    acc[:n] = y
            elif j < T - 1:
                acc[:n] += term(j)
            else:
                xout[rows] = (acc[:n] + term(j) + xin[rows].astype(f32)).astype(bf)

        @pl.when(s < last)
        def _():
            x_copy(c).start()

    def send_A(m):
        for k in range(1, N):
            A_copy(m, k).start()
        owner, cols = in_block(d)
        A[m, 0] = xg[owner, pl.ds(m * R, R), cols]

    def bwd(c, is_last):
        m, start, n = chunks[c]
        rows = rows_at(c)
        if is_last:
            gin[rows] = (cv[rows].astype(f32) * xout[rows].astype(f32)).astype(bf)
        else:
            g_copy(c).wait_recv()
        g = gin[rows]
        G[m, 0, pl.ds(start, n)] = clip(g, lim_g)
        own_sends(lambda to, ss: G_copy(c, d, to, ss).start())
        gmax[...] = jnp.maximum(gmax[...], fold(g))

        def settle(j):
            level = 0
            while not (j >> level) & 1:
                rd_copy(c, j ^ stages[level], level).wait_recv()
                part[j, rows] = (part[j, rows].astype(f32) + rs[level, j, rows].astype(f32)).astype(bf)
                level += 1
            rd_copy(c, j, level).start()

        for j in reversed(range(T)):
            y = jnp.dot(G[m, 0, pl.ds(start, n)], wt[t ^ j], preferred_element_type=f32)
            part[j, rows] = y.astype(bf)
            if j & 1:
                rd_copy(c, j, 0).start()
                if j + 1 < T:
                    settle(j + 1)

    def finb(c):
        rows = rows_at(c)
        total = gin[rows].astype(f32) + part[0, rows].astype(f32)
        for level in range(len(stages)):
            rd_copy(c, stages[level], level).wait_recv()
            total = total + rs[level, 0, rows].astype(f32)
        gout[rows] = total.astype(bf)

        @pl.when(s > 0)
        def _():
            g_copy(c).start()

    def relay_G(c):
        relays(lambda origin: G_wait(c, origin), lambda origin, to, ss: G_copy(c, origin, to, ss).start())

    def arrive_G(c):
        for step in range(1, N):
            for way in (1, -1):
                origin = d - way * step
                here = inside(origin)
                if step % 2 == 0:
                    here = here & ~inside(d + way)

                @pl.when(here)
                def _(origin=origin):
                    G_wait(c, origin)

    def relay_A(m):
        there = A.at[m, pl.ds(1, N - 1), rows_of(t)]
        remote(there, there, A_ss, A_rs.at[m], dp=d ^ 1).wait_recv()
        for st in strides_below(0, T):
            B_copy(m, 0, st).start()

    def relay_B(m):
        for j in range(1, T):
            if strides_below(j, T):
                B_arrival(m, j).wait_recv()
                for st in strides_below(j, T):
                    B_copy(m, j, st).start()

    def turn_A(m):
        for j in range(1, T):
            if not strides_below(j, T):
                B_arrival(m, j).wait_recv()
        for k in range(N):
            def body(i, _, k=k):
                cols = pl.ds(pl.multiple_of(i * 128, 128), 128)
                At[m, cols, pl.ds(k * R, R)] = A[m, k, :, cols].T
                return 0

            lax.fori_loop(0, FA // 128, body, 0)

    def update(m):
        def body(n, _):
            rows = pl.ds(pl.multiple_of(n * 128, 128), 128)
            y = jnp.dot(At[m, rows], G[m].reshape(N * R, F), preferred_element_type=f32)
            if m == 0:
                dw[rows] = y
            else:
                dw[rows] += y
            return 0

        lax.fori_loop(0, FA // 128, body, 0)

    def peers():
        return [(k, j) for k in range(N) for j in range(T) if k or j]

    def p_copy(k, j):
        i = k * T + j
        return remote(pk.at[0], pk.at[i], p_ss, p_rs, dp=d ^ k, tensor=t ^ j)

    def send_peaks():
        row = lax.broadcasted_iota(jnp.int32, (8, 128), 0)
        top_a = jnp.max(amax[...].astype(f32), keepdims=True).reshape(1, 1)
        top_g = jnp.max(gmax[...].astype(f32), keepdims=True).reshape(1, 1)
        pk[0] = jnp.where(row == 0, top_a, jnp.where(row == 1, w_peak, top_g))
        for k, j in peers():
            p_copy(k, j).start()

    ends = [max(c for c in range(NC) if chunks[c][0] == m) for m in range(M)]

    def meet(first, end):
        for r in range(first, end):
            greeted(r)
            if r + 1 < N - 2:
                greet(r + 1)

    enter()
    greet(0)

    @pl.when(s == 0)
    def _():
        prep(0)
        prep(1)

    w_peak = clip_weights()

    @pl.when(s > 0)
    def _():
        turn_weights()
        meet(0, N - 2)
        prep(0)
        prep(1)

    def arrive(m):
        for c in range(NC):
            if chunks[c][0] == m:
                arrive_G(c)

    @pl.when(s == last)
    def _():
        cot_load.wait()
        for c in range(NC):
            fwd(c)
            if c in ends:
                send_A(ends.index(c))
            bwd(c, True)
            if c == NC - 1:
                send_peaks()
            if c + 2 < NC:
                prep(c + 2)
            if c:
                finb(c - 1)
            if c >= 2:
                relay_G(c - 2)
        finb(NC - 1)
        for m in range(M - 1):
            relay_A(m)
        relay_G(NC - 2)
        relay_A(M - 1)
        for m in range(M - 1):
            relay_B(m)
            turn_A(m)
            arrive(m)
            update(m)
        relay_B(M - 1)
        relay_G(NC - 1)
        turn_A(M - 1)

    @pl.when(s < last)
    def _():
        for c in range(NC):
            fwd(c)
            if c + 2 < NC:
                prep(c + 2)
            if c < 2:
                @pl.when(s == 0)
                def _(c=c):
                    meet(max(0, N - 3) * c, N - 3 + c)
            if c in ends:
                send_A(ends.index(c))

        @pl.when(s == 0)
        def _():
            turn_weights()

        relay_A(0)
        for c in range(NC):
            bwd(c, False)
            if c == NC - 1:
                send_peaks()
            if c:
                finb(c - 1)
            if c < M - 1:
                relay_A(c + 1)
            if 1 <= c <= M:
                relay_B(c - 1)
            if c >= 2:
                relay_G(c - 2)
            if 2 <= c < M + 2:
                turn_A(c - 2)
        relay_G(NC - 2)
        finb(NC - 1)
        for m in range(M - 1):
            arrive(m)
            update(m)
        relay_G(NC - 1)

    arrive(M - 1)

    def peakwait():
        there = pk.at[pl.ds(1, N * T - 1)]
        remote(there, there, p_ss, p_rs, dp=d ^ 1).wait_recv()
        out_top[...] = jnp.max(pk[...], axis=0)

    def sent(ref, sem):
        remote(ref, ref, sem, p_rs, dp=d ^ 1).wait_send()

    def finalwait():
        most = pl.ds(0, T - 1)
        sent(xg.at[most], ag_ss)
        sent(part.at[most], rd_ss)
        own_sends(lambda to, ss: sent(gin, ss))
        relays(lambda origin: None, lambda origin, to, ss: sent(gin, ss))

        @pl.when(s < last)
        def _():
            sent(gin, x_ss)

        @pl.when(s > 0)
        def _():
            sent(gin, g_ss)

        sent(A.at[:, pl.ds(1, N - 1), rows_of(t)], A_ss)
        sent(A.at[:, pl.ds(1, N - 1), pl.ds(0, (T - 1) * piece)], B_ss)
        sent(pk.at[pl.ds(1, N * T - 1)], p_ss)

    peakwait()
    finalwait()


def finish(M, tile, acts, grads, G, At, dw, top, hist_a, hist_w, hist_g,
           out_acts, out_grads, out_w, out_ha, out_hw, out_hg, held, hv, hn, sem, w_sem, h_sem, n_sem):
    moves = [pltpu.make_async_copy(acts, out_acts, sem.at[0]),
             pltpu.make_async_copy(grads, out_grads, sem.at[1])]
    loads = [pltpu.make_async_copy(h, hv.at[i], h_sem.at[i]) for i, h in enumerate((hist_a, hist_w, hist_g))]
    for copy in moves + loads:
        copy.start()
    count, width = dw.shape[0] // tile, dw.shape[1]
    outs = []
    for n in range(count):
        rows = pl.ds(n * tile, tile)
        y = jnp.dot(At[M - 1, rows], G[M - 1].reshape(-1, width), preferred_element_type=jnp.float32)
        if M > 1:
            y = dw[rows] + y
        held[rows] = y.astype(held.dtype)
        outs.append(pltpu.make_async_copy(held.at[rows], out_w.at[rows], w_sem.at[n]))
        outs[-1].start()
    peaks = top[...]
    for row, out in enumerate((out_ha, out_hw, out_hg)):
        loads[row].wait()
        hn[row] = jnp.concatenate([peaks[row:row + 1, 0:1], hv[row][:, :-1]], axis=1)
        copy = pltpu.make_async_copy(hn.at[row], out, n_sem.at[row])
        copy.start()
        moves.append(copy)
    for copy in moves + outs:
        copy.wait()


def shards(acts_in, weights, cotangent, hist_act, hist_weight, hist_grad):
    S, N, T = lax.axis_size("pipe"), lax.axis_size("dp"), lax.axis_size("tensor")
    M, R, F = acts_in.shape
    chunks = chunks_of(M, R)
    NC, RT = len(chunks), M * R
    FA = T * F // N
    bf, f32 = jnp.bfloat16, jnp.float32
    levels = max(1, T.bit_length() - 1)
    dma = pltpu.SemaphoreType.DMA
    hbm = pl.BlockSpec(memory_space=pltpu.HBM)
    vmem = pl.BlockSpec(memory_space=pltpu.VMEM)
    flat = (RT, F)
    H = hist_act.shape
    hist = jax.ShapeDtypeStruct(H, f32)
    half = max(1, (N + 1) // 2 - 1)
    acts, grads, G, At, dw, top = pl.pallas_call(
        functools.partial(kernel, S, N, T, M, R, F, FA, chunks),
        out_shape=(pltpu.VMEM(flat, bf), pltpu.VMEM(flat, bf),
                   pltpu.VMEM((M, N, R, F), bf), pltpu.VMEM((M, FA, N * R), bf),
                   pltpu.VMEM((FA, F), f32), pltpu.VMEM((8, 128), f32)),
        in_specs=[hbm] * 6,
        out_specs=(vmem,) * 6,
        scratch_shapes=[
            pltpu.VMEM((T, F, F), bf),
            pltpu.VMEM((T, F, F), bf),
            pltpu.VMEM((3,) + H, f32),
            pltpu.VMEM(flat, bf),
            pltpu.VMEM(flat, bf),
            pltpu.VMEM((T,) + flat, bf),
            pltpu.VMEM((max(n for _, _, n in chunks), F), f32),
            pltpu.VMEM(flat, bf),
            pltpu.VMEM((T,) + flat, bf),
            pltpu.VMEM((levels, T) + flat, bf),
            pltpu.VMEM((M, N, R, FA), bf),
            pltpu.VMEM((N * T, 8, 128), f32),
            pltpu.VMEM((16, F), bf),
            pltpu.VMEM((16, F), bf),
            dma((T,)), dma(()), dma((2,)), dma(()), dma(()), dma((NC,)), dma(()), dma((NC, T - 1)),
            dma(()), dma((NC,)), dma(()), dma((NC, T - 1)),
            dma((4,)), dma((NC, N - 1)), dma((2, half, 2)),
            dma(()), dma((M,)), dma(()), dma((M, T - 1)),
            dma(()), dma(()), pltpu.SemaphoreType.REGULAR((max(1, N - 2), 2)),
        ],
        compiler_params=pltpu.CompilerParams(
            collective_id=0, has_side_effects=True, vmem_limit_bytes=40 * 2**20),
    )(*(pltpu.with_memory_space_constraint(v, pltpu.HBM) for v in (
        acts_in.reshape(flat), weights.reshape(T, F, F), cotangent.reshape(flat),
        hist_act, hist_weight, hist_grad)))

    def hold(v):
        return pltpu.with_memory_space_constraint(v, pltpu.VMEM)

    tile = min(256, FA)
    out_acts, out_grads, out_w, ha, hw, hg = pl.pallas_call(
        functools.partial(finish, M, tile),
        out_shape=(jax.ShapeDtypeStruct(flat, bf), jax.ShapeDtypeStruct(flat, bf),
                   jax.ShapeDtypeStruct((FA, F), bf), hist, hist, hist),
        in_specs=[vmem] * 6 + [hbm] * 3,
        out_specs=(hbm,) * 6,
        scratch_shapes=[pltpu.VMEM((FA, F), bf), pltpu.VMEM((3,) + H, f32), pltpu.VMEM((3,) + H, f32),
                        dma((2,)), dma((FA // tile,)), dma((3,)), dma((3,))],
        compiler_params=pltpu.CompilerParams(vmem_limit_bytes=16 * 2**20),
    )(*(hold(v) for v in (acts, grads, G, At, dw, top)), hist_act, hist_weight, hist_grad)
    full = (1, M, R, F)
    return out_acts.reshape(full), out_grads.reshape(full), out_w[None], ha, hw, hg


def solution(mesh):
    placed = (P(None, "dp", "tensor"), P("pipe", None, "tensor"), P(None, "dp", "tensor"),
              P("pipe", None), P("pipe", None), P("pipe", None))
    return jax.shard_map(
        shards, mesh=mesh, in_specs=placed,
        out_specs=(P("pipe", None, "dp", "tensor"), P("pipe", None, "dp", "tensor"),
                   P("pipe", "dp", "tensor"), P("pipe", None), P("pipe", None), P("pipe", None)),
        check_vma=False)
```

```python
import functools

import jax
import jax.numpy as jnp
from jax import lax
from jax.experimental import pallas as pl
from jax.experimental.pallas import tpu as pltpu
from jax.sharding import PartitionSpec as P

MESH = pl.DeviceIdType.MESH
PARTS = 8
FIRST, LATER = (2, 3, 3), (4, 4)


def strides_below(index, count):
    low = (index & -index) if index else count
    step, found = low // 2, []
    while step:
        found.append(step)
        step //= 2
    return found


def low(i):
    return i & -i


def chunks_of(M, R):
    found = []
    for m in range(M):
        start = 0
        for part in FIRST if m == 0 else LATER:
            found.append((m, start, R * part // PARTS))
            start += R * part // PARTS
    return found


def kernel(S, N, T, M, R, F, FA, chunks,
           acts, weights, cot, hist_a, hist_w, hist_g,
           xout, gout, G, At, dw, out_top,
           w, wt, hv, cv, xin, xg, acc, gin, part, rs, A, pk, amax, gmax, gd, gh,
           w_sem, h_sem, in_sem, c_sem, x_ss, x_rs, ag_ss, ag_rs, g_ss, g_rs, rd_ss, rd_rs,
           G_ss, G_rs, Gr_ss, Gm_ss, A_ss, A_rs, B_ss, B_rs, p_ss, p_rs, hello, ready,
           gd_ss, gd_rs):
    s, d, t = lax.axis_index("pipe"), lax.axis_index("dp"), lax.axis_index("tensor")
    last = S - 1
    bf, f32 = jnp.bfloat16, jnp.float32
    NC = len(chunks)
    top = T // 2
    stages = []
    st = 1
    while st < T:
        stages.append(st)
        st *= 2

    def remote(src, dst, ss, rsem, **where):
        return pltpu.make_async_remote_copy(
            src_ref=src, dst_ref=dst, send_sem=ss, recv_sem=rsem,
            device_id=where, device_id_type=MESH)

    def signal(sem, **where):
        pl.semaphore_signal(sem, inc=1, device_id=where, device_id_type=MESH)

    barrier = pltpu.get_barrier_semaphore()
    for st in stages:
        signal(barrier, tensor=t ^ st)

    @pl.when(s > 0)
    def _():
        signal(barrier, pipe=s - 1)

    @pl.when(s < last)
    def _():
        signal(barrier, pipe=s + 1)

    @pl.when(d > 0)
    def _():
        signal(barrier, dp=d - 1)

    @pl.when(d < N - 1)
    def _():
        signal(barrier, dp=d + 1)

    def rows_at(c):
        m, start, n = chunks[c]
        return pl.ds(m * R + start, n)

    h_loads = [pltpu.make_async_copy(h, hv.at[i], h_sem)
               for i, h in enumerate((hist_a, hist_w, hist_g))]
    loads = [pltpu.make_async_copy(weights.at[b], w.at[b], w_sem.at[b]) for b in range(T)]
    first = chunks[0][2]
    in_loads = [pltpu.make_async_copy(acts.at[rows], xin.at[rows], in_sem.at[i])
                for i, rows in enumerate((pl.ds(0, first), pl.ds(first, M * R - first)))]
    cot_load = pltpu.make_async_copy(cot, cv, c_sem)
    for copy in h_loads:
        copy.start()

    @pl.when(s == 0)
    def _():
        for copy in in_loads:
            copy.start()

    pltpu.make_async_copy(hv, hv, h_sem).wait()
    for copy in loads:
        copy.start()

    @pl.when(s == last)
    def _():
        cot_load.start()

    def limit(i):
        return jnp.max(hv[i], axis=1, keepdims=True).astype(bf)

    lim_a, lim_w, lim_g = limit(0), limit(1), limit(2)

    def clip(v, lim):
        return jnp.minimum(jnp.maximum(v, -lim), lim)

    def fold(v):
        return jnp.max(jnp.abs(v).reshape(-1, 16, v.shape[-1]), axis=0)

    amax[...] = jnp.zeros_like(amax)
    gmax[...] = jnp.zeros_like(gmax)

    def enter():
        near = (s > 0).astype(jnp.int32) + (s < last).astype(jnp.int32)
        beside = (d > 0).astype(jnp.int32) + (d < N - 1).astype(jnp.int32)
        pl.semaphore_wait(barrier, len(stages) + near + beside)

    def greet(r):
        @pl.when(d > 0)
        def _():
            signal(hello.at[r, 0], dp=d - 1)

        @pl.when(d < N - 1)
        def _():
            signal(hello.at[r, 1], dp=d + 1)

    def greeted(r):
        @pl.when(d < N - 1)
        def _():
            pl.semaphore_wait(hello.at[r, 0], 1)

        @pl.when(d > 0)
        def _():
            pl.semaphore_wait(hello.at[r, 1], 1)

    up = jnp.minimum(s + 1, last)
    down = jnp.maximum(s - 1, 0)

    def gd_copy(c):
        return remote(part.at[top, rows_at(c)], gd.at[rows_at(c)], gd_ss, gd_rs.at[c], pipe=down, tensor=t ^ top)

    def x_copy(c):
        return remote(xout.at[rows_at(c)], xin.at[rows_at(c)], x_ss, x_rs.at[c], pipe=up)

    def g_copy(c):
        return remote(gh.at[rows_at(c)], gin.at[rows_at(c)], g_ss, g_rs.at[c], pipe=down)

    def ag_copy(c, j, st):
        i = j ^ st
        return remote(xg.at[j, rows_at(c)], xg.at[i, rows_at(c)], ag_ss, ag_rs.at[c, i - 1], tensor=t ^ st)

    def G_copy(c, origin, to, ss):
        m, start, n = chunks[c]
        rows = pl.ds(start, n)
        return remote(G.at[m, origin ^ d, rows], G.at[m, origin ^ to, rows], ss, G_rs.at[c, (origin ^ to) - 1], dp=to)

    def G_wait(c, origin):
        m, start, n = chunks[c]
        here = G.at[m, origin ^ d, pl.ds(start, n)]
        remote(here, here, G_ss.at[0], G_rs.at[c, (origin ^ d) - 1], dp=origin).wait_recv()

    def inside(at):
        return (at >= 0) & (at < N)

    def own_sends(act, mix=False):
        for i, step in enumerate((2, -2, 1, -1)):
            if abs(step) < N:
                here = inside(d + step)
                if mix and abs(step) == 2:
                    here = here & inside(d + step + step // 2)

                @pl.when(here)
                def _(i=i, to=d + step):
                    act(to, G_ss.at[i])

    def near_end(way):
        return inside(d - way) & inside(d + way) & ~inside(d + 2 * way)

    def relays(wait, act, mix=False):
        for i, way in enumerate((1, -1)):
            if mix:
                @pl.when(near_end(way))
                def _(i=i, way=way):
                    wait(d - way)
                    act(d - way, d + way, Gm_ss.at[i])

            for m in range(1, (N + 1) // 2):
                origin = d - way * 2 * m

                @pl.when(inside(origin) & inside(d + way))
                def _(i=i, way=way, m=m, origin=origin):
                    wait(origin)
                    for step in (1, 2):
                        if 2 * m + step < N:
                            @pl.when(inside(d + way * step))
                            def _(step=step):
                                act(origin, d + way * step, Gr_ss.at[i, m - 1, step - 1])

    ratio = N // T

    def in_block(r):
        start = lax.rem(r, ratio) * FA
        return t ^ lax.div(r, ratio), pl.ds(pl.multiple_of(start, FA), FA)

    piece = FA // T

    def cols_of(owner):
        return pl.ds(pl.multiple_of(owner * piece, piece), piece)

    def A_copy(c, k):
        m, start, n = chunks[c]
        r = d ^ k
        cols = pl.ds(pl.multiple_of(lax.rem(r, ratio) * FA + t * piece, piece), piece)
        return remote(xg.at[t ^ lax.div(r, ratio), rows_at(c), cols], A.at[m, k, pl.ds(start, n), cols_of(t)],
                      A_ss, A_rs.at[m], dp=r)

    def B_copy(m, j, st):
        i = j ^ st
        there = A.at[m, pl.ds(1, N - 1), :, cols_of(t ^ j)]
        return remote(there, there, B_ss, B_rs.at[m, i - 1], tensor=t ^ st)

    def B_arrival(m, i):
        there = A.at[m, pl.ds(1, N - 1), :, cols_of(t ^ i)]
        return remote(there, there, B_ss, B_rs.at[m, i - 1], tensor=t ^ low(i))

    def rd_copy(c, j, level):
        st = stages[level]
        i = j ^ st
        return remote(part.at[j, rows_at(c)], rs.at[level, i, rows_at(c)], rd_ss, rd_rs.at[c, i + st - 1],
                      tensor=t ^ st)

    def prep(c):
        rows = rows_at(c)

        @pl.when(s == 0)
        def _():
            if c < len(in_loads):
                in_loads[c].wait()

        @pl.when(s > 0)
        def _():
            x_copy(c).wait_recv()

        x = xin[rows]
        xg[0, rows] = clip(x, lim_a)
        for st in strides_below(0, T):
            ag_copy(c, 0, st).start()
        amax[...] = jnp.maximum(amax[...], fold(x))

    def clip_weights():
        peak = jnp.zeros((16, F), bf)
        for b in range(T):
            loads[b].wait()

            def body(i, m, b=b):
                rows = pl.ds(pl.multiple_of(i * 128, 128), 128)
                v = w[b, rows]
                w[b, rows] = clip(v, lim_w)
                return jnp.maximum(m, fold(v))

            peak = lax.fori_loop(0, F // 128, body, peak)
        return jnp.max(peak.astype(f32), keepdims=True).reshape(1, 1)

    def turn_weights(first, end):
        for b in range(first, end):
            def body(i, _, b=b):
                rows = pl.ds(pl.multiple_of(i * 128, 128), 128)
                wt[b, :, rows] = w[b, rows].T
                return 0

            lax.fori_loop(0, F // 128, body, 0)

    def fwd(c):
        rows = rows_at(c)
        n = chunks[c][2]

        def term(j):
            return jnp.dot(xg[j, rows], w[t ^ j], preferred_element_type=f32)

        for j in range(T):
            if j:
                ag_copy(c, j ^ low(j), low(j)).wait_recv()
                for st in strides_below(j, T):
                    ag_copy(c, j, st).start()
            if j == 0:
                if T == 1:
                    xout[rows] = (term(0) + xin[rows].astype(f32)).astype(bf)
            elif j == 1:
                y = term(0) + term(1)
                if T == 2:
                    xout[rows] = (y + xin[rows].astype(f32)).astype(bf)
                else:
                    acc[:n] = y
            elif j < T - 1:
                acc[:n] += term(j)
            else:
                xout[rows] = (acc[:n] + term(j) + xin[rows].astype(f32)).astype(bf)

        if c == 0 and top:
            pl.semaphore_wait(ready, 1)

        @pl.when(s < last)
        def _():
            x_copy(c).start()

    def send_A(c):
        m, start, n = chunks[c]
        for k in range(1, N):
            A_copy(c, k).start()
        owner, cols = in_block(d)
        A[m, 0, pl.ds(start, n)] = xg[owner, rows_at(c), cols]

    def bwd(c, is_last):
        m, start, n = chunks[c]
        rows = rows_at(c)
        if is_last:
            gin[rows] = (cv[rows].astype(f32) * xout[rows].astype(f32)).astype(bf)
        else:
            g_copy(c).wait_recv()
            if top:
                gd_copy(c).wait_recv()
                gin[rows] = (gin[rows].astype(f32) + gd[rows].astype(f32)).astype(bf)
        g = gin[rows]
        G[m, 0, pl.ds(start, n)] = clip(g, lim_g)
        if c == NC - 1:
            gmax[...] = jnp.maximum(gmax[...], fold(g))
            send_peaks()
        send_G(c, is_last)
        if c < NC - 1:
            gmax[...] = jnp.maximum(gmax[...], fold(g))

        def settle(j):
            level = 0
            while not (j >> level) & 1:
                rd_copy(c, j ^ stages[level], level).wait_recv()
                part[j, rows] = (part[j, rows].astype(f32) + rs[level, j, rows].astype(f32)).astype(bf)
                level += 1
            rd_copy(c, j, level).start()
            if j == top:
                @pl.when(s > 0)
                def _():
                    gd_copy(c).start()

        def term(j):
            return jnp.dot(G[m, 0, pl.ds(start, n)], wt[t ^ j], preferred_element_type=f32).astype(bf)

        for j in reversed(range(1, T, 2)):
            y, z = term(j), term(j - 1)
            part[j, rows] = y
            part[j - 1, rows] = z
            rd_copy(c, j, 0).start()
            if j + 1 < T:
                settle(j + 1)
        if T == 1:
            part[0, rows] = term(0)

    def pass_on(c):
        rows = rows_at(c)

        @pl.when(s > 0)
        def _():
            total = gin[rows].astype(f32) + part[0, rows].astype(f32)
            for level in range(len(stages) - 1):
                rd_copy(c, stages[level], level).wait_recv()
                total = total + rs[level, 0, rows].astype(f32)
            gh[rows] = total.astype(bf)
            g_copy(c).start()

    def mixed(c, is_last):
        return is_last and M > 1 and 0 < c and chunks[c][0] == 0

    def send_G(c, is_last):
        own_sends(lambda to, ss: G_copy(c, d, to, ss).start(), mixed(c, is_last))

    def finb(c):
        rows = rows_at(c)
        total = gin[rows].astype(f32) + part[0, rows].astype(f32)
        for level in range(len(stages)):
            if level < len(stages) - 1:
                @pl.when(s == 0)
                def _(level=level):
                    rd_copy(c, stages[level], level).wait_recv()
            else:
                rd_copy(c, stages[level], level).wait_recv()
            total = total + rs[level, 0, rows].astype(f32)
        gout[rows] = total.astype(bf)

    def relay_G(c, is_last=False):
        relays(lambda origin: G_wait(c, origin), lambda origin, to, ss: G_copy(c, origin, to, ss).start(),
               mixed(c, is_last))

    def arrive_G(c, is_last=False):
        for step in range(1, N):
            for way in (1, -1):
                origin = d - way * step
                here = inside(origin)
                if step % 2 == 0:
                    here = here & ~inside(d + way)
                elif step == 1 and mixed(c, is_last):
                    here = here & ~near_end(way)

                @pl.when(here)
                def _(origin=origin):
                    G_wait(c, origin)

    def relay_A(m):
        there = A.at[m, pl.ds(1, N - 1), :, cols_of(t)]
        remote(there, there, A_ss, A_rs.at[m], dp=d ^ 1).wait_recv()
        for st in strides_below(0, T):
            B_copy(m, 0, st).start()

    def relay_B(m):
        for j in range(1, T):
            if strides_below(j, T):
                B_arrival(m, j).wait_recv()
                for st in strides_below(j, T):
                    B_copy(m, j, st).start()

    def turn_A(m):
        for j in range(1, T):
            if not strides_below(j, T):
                B_arrival(m, j).wait_recv()
        for k in range(N):
            def body(i, _, k=k):
                cols = pl.ds(pl.multiple_of(i * 128, 128), 128)
                At[m, cols, pl.ds(k * R, R)] = A[m, k, :, cols].T
                return 0

            lax.fori_loop(0, FA // 128, body, 0)

    def update(m):
        tile = min(256, FA)

        def body(n, _):
            rows = pl.ds(pl.multiple_of(n * tile, tile), tile)
            y = jnp.dot(At[m, rows], G[m].reshape(N * R, F), preferred_element_type=f32)
            if m == 0:
                dw[rows] = y
            else:
                dw[rows] += y
            return 0

        lax.fori_loop(0, FA // tile, body, 0)

    def peers():
        return [(k, j) for k in range(N) for j in range(T) if k or j]

    def p_copy(k, j):
        i = k * T + j
        return remote(pk.at[0], pk.at[i], p_ss, p_rs, dp=d ^ k, tensor=t ^ j)

    def send_peaks():
        row = lax.broadcasted_iota(jnp.int32, (8, 128), 0)
        top_a = jnp.max(amax[...].astype(f32), keepdims=True).reshape(1, 1)
        top_g = jnp.max(gmax[...].astype(f32), keepdims=True).reshape(1, 1)
        pk[0] = jnp.where(row == 0, top_a, jnp.where(row == 1, w_peak, top_g))
        for k, j in peers():
            p_copy(k, j).start()

    ends = [max(c for c in range(NC) if chunks[c][0] == m) for m in range(M)]

    def meet(first, end):
        for r in range(first, end):
            greeted(r)
            if r + 1 < N - 2:
                greet(r + 1)

    enter()
    greet(0)
    if top:
        signal(ready, tensor=t ^ top)

    @pl.when(s == 0)
    def _():
        prep(0)
        prep(1)

    w_peak = clip_weights()

    @pl.when(s > 0)
    def _():
        meet(0, 1)
        turn_weights(0, T)
        prep(0)
        prep(1)
        meet(1, N - 2)

    def arrive(m, is_last=False):
        for c in range(NC):
            if chunks[c][0] == m:
                arrive_G(c, is_last)

    @pl.when(s == last)
    def _():
        cot_load.wait()
        for c in range(NC):
            fwd(c)
            send_A(c)
            bwd(c, True)
            if c + 2 < NC:
                prep(c + 2)
            if c == 1:
                relay_G(0, True)
            if c >= 3:
                relay_G(c - 2, True)
            pass_on(c)
            if c >= 2:
                finb(c - 2)
        for c in range(max(0, NC - 2), NC):
            finb(c)
        relay_G(NC - 2, True)
        for m in range(M):
            relay_A(m)
            if m:
                arrive(m - 1, True)
                update(m - 1)
            relay_B(m)
            if m == M - 1:
                relay_G(NC - 1, True)
            turn_A(m)

    @pl.when(s < last)
    def _():
        for c in range(NC):
            fwd(c)
            if c + 2 < NC:
                prep(c + 2)
            if c < 2:
                @pl.when(s == 0)
                def _(c=c):
                    meet(max(0, N - 3) * c, N - 3 + c)
            if c:
                for b in range(0 if c == 1 else c, c + 1):
                    send_A(b)

                @pl.when(s == 0)
                def _(c=c):
                    turn_weights(T * c // NC if c > 1 else 0, T * (c + 1) // NC)

        relay_A(0)
        for c in range(NC):
            if c >= 2:
                relay_G(c - 1)
            bwd(c, False)
            pass_on(c)
            if c == 1:
                relay_G(0)
            if 1 <= c < M:
                relay_A(c)
            if c >= 2:
                finb(c - 2)
                if c - 2 < M:
                    relay_B(c - 2)
            if 3 <= c < M + 3:
                turn_A(c - 3)
        for c in range(max(0, NC - 2), NC - 1):
            finb(c)
        relay_G(NC - 1)
        finb(NC - 1)
        for m in range(M - 1):
            arrive(m)
            update(m)

    arrive(M - 1)

    def peakwait():
        there = pk.at[pl.ds(1, N * T - 1)]
        remote(there, there, p_ss, p_rs, dp=d ^ 1).wait_recv()
        out_top[...] = jnp.max(pk[...], axis=0)

    def sent(ref, sem):
        remote(ref, ref, sem, p_rs, dp=d ^ 1).wait_send()

    def finalwait():
        if top:
            sent(xg.at[pl.ds(0, T - 1)], ag_ss)
            sent(part.at[pl.ds(0, T - 1)], rd_ss)

            @pl.when(s > 0)
            def _():
                sent(gin, gd_ss)

        def own_sent(to, ss):
            sent(gin, ss)

        @pl.when(s < last)
        def _():
            own_sends(own_sent)

        @pl.when(s == last)
        def _():
            if M > 1:
                own_sends(lambda to, ss: sent(gin.at[pl.ds(0, R - first)], ss), True)
                own_sends(lambda to, ss: sent(gin.at[pl.ds(R - first, (M - 1) * R + first)], ss))
                for i, way in enumerate((1, -1)):
                    @pl.when(near_end(way))
                    def _(i=i):
                        sent(gin.at[pl.ds(0, R - first)], Gm_ss.at[i])
            else:
                own_sends(own_sent)

        relays(lambda origin: None, lambda origin, to, ss: sent(gin, ss))

        @pl.when(s < last)
        def _():
            sent(gin, x_ss)

        @pl.when(s > 0)
        def _():
            sent(gin, g_ss)

        sent(A.at[:, pl.ds(1, N - 1), :, cols_of(t)], A_ss)
        sent(A.at[:, pl.ds(1, N - 1), :, pl.ds(0, (T - 1) * piece)], B_ss)
        sent(pk.at[pl.ds(1, N * T - 1)], p_ss)

    peakwait()
    finalwait()


def finish(M, tile, acts, grads, G, At, dw, top, hist_a, hist_w, hist_g,
           out_acts, out_grads, out_w, out_ha, out_hw, out_hg, held, hv, hn, sem, w_sem, h_sem, n_sem):
    moves = [pltpu.make_async_copy(acts, out_acts, sem.at[0]),
             pltpu.make_async_copy(grads, out_grads, sem.at[1])]
    loads = [pltpu.make_async_copy(h, hv.at[i], h_sem.at[i]) for i, h in enumerate((hist_a, hist_w, hist_g))]
    for copy in moves + loads:
        copy.start()
    count, width = dw.shape[0] // tile, dw.shape[1]
    outs = []
    for n in range(count):
        rows = pl.ds(n * tile, tile)
        y = jnp.dot(At[M - 1, rows], G[M - 1].reshape(-1, width), preferred_element_type=jnp.float32)
        if M > 1:
            y = dw[rows] + y
        held[rows] = y.astype(held.dtype)
        outs.append(pltpu.make_async_copy(held.at[rows], out_w.at[rows], w_sem.at[n]))
        outs[-1].start()
    peaks = top[...]
    for row, out in enumerate((out_ha, out_hw, out_hg)):
        loads[row].wait()
        hn[row] = jnp.concatenate([peaks[row:row + 1, 0:1], hv[row][:, :-1]], axis=1)
        copy = pltpu.make_async_copy(hn.at[row], out, n_sem.at[row])
        copy.start()
        moves.append(copy)
    for copy in moves + outs:
        copy.wait()


def shards(acts_in, weights, cotangent, hist_act, hist_weight, hist_grad):
    S, N, T = lax.axis_size("pipe"), lax.axis_size("dp"), lax.axis_size("tensor")
    M, R, F = acts_in.shape
    chunks = chunks_of(M, R)
    NC, RT = len(chunks), M * R
    FA = T * F // N
    bf, f32 = jnp.bfloat16, jnp.float32
    levels = max(1, T.bit_length() - 1)
    dma = pltpu.SemaphoreType.DMA
    hbm = pl.BlockSpec(memory_space=pltpu.HBM)
    vmem = pl.BlockSpec(memory_space=pltpu.VMEM)
    flat = (RT, F)
    H = hist_act.shape
    hist = jax.ShapeDtypeStruct(H, f32)
    half = max(1, (N + 1) // 2 - 1)
    acts, grads, G, At, dw, top = pl.pallas_call(
        functools.partial(kernel, S, N, T, M, R, F, FA, chunks),
        out_shape=(pltpu.VMEM(flat, bf), pltpu.VMEM(flat, bf),
                   pltpu.VMEM((M, N, R, F), bf), pltpu.VMEM((M, FA, N * R), bf),
                   pltpu.VMEM((FA, F), f32), pltpu.VMEM((8, 128), f32)),
        in_specs=[hbm] * 6,
        out_specs=(vmem,) * 6,
        scratch_shapes=[
            pltpu.VMEM((T, F, F), bf),
            pltpu.VMEM((T, F, F), bf),
            pltpu.VMEM((3,) + H, f32),
            pltpu.VMEM(flat, bf),
            pltpu.VMEM(flat, bf),
            pltpu.VMEM((T,) + flat, bf),
            pltpu.VMEM((max(n for _, _, n in chunks), F), f32),
            pltpu.VMEM(flat, bf),
            pltpu.VMEM((T,) + flat, bf),
            pltpu.VMEM((levels, T) + flat, bf),
            pltpu.VMEM((M, N, R, FA), bf),
            pltpu.VMEM((N * T, 8, 128), f32),
            pltpu.VMEM((16, F), bf),
            pltpu.VMEM((16, F), bf),
            pltpu.VMEM(flat, bf),
            pltpu.VMEM(flat, bf),
            dma((T,)), dma(()), dma((2,)), dma(()), dma(()), dma((NC,)), dma(()), dma((NC, T - 1)),
            dma(()), dma((NC,)), dma(()), dma((NC, T - 1)),
            dma((4,)), dma((NC, N - 1)), dma((2, half, 2)), dma((2,)),
            dma(()), dma((M,)), dma(()), dma((M, T - 1)),
            dma(()), dma(()), pltpu.SemaphoreType.REGULAR((max(1, N - 2), 2)),
            pltpu.SemaphoreType.REGULAR, dma(()), dma((NC,)),
        ],
        compiler_params=pltpu.CompilerParams(
            collective_id=0, has_side_effects=True, vmem_limit_bytes=40 * 2**20),
    )(*(pltpu.with_memory_space_constraint(v, pltpu.HBM) for v in (
        acts_in.reshape(flat), weights.reshape(T, F, F), cotangent.reshape(flat),
        hist_act, hist_weight, hist_grad)))

    def hold(v):
        return pltpu.with_memory_space_constraint(v, pltpu.VMEM)

    tile = min(256, FA)
    out_acts, out_grads, out_w, ha, hw, hg = pl.pallas_call(
        functools.partial(finish, M, tile),
        out_shape=(jax.ShapeDtypeStruct(flat, bf), jax.ShapeDtypeStruct(flat, bf),
                   jax.ShapeDtypeStruct((FA, F), bf), hist, hist, hist),
        in_specs=[vmem] * 6 + [hbm] * 3,
        out_specs=(hbm,) * 6,
        scratch_shapes=[pltpu.VMEM((FA, F), bf), pltpu.VMEM((3,) + H, f32), pltpu.VMEM((3,) + H, f32),
                        dma((2,)), dma((FA // tile,)), dma((3,)), dma((3,))],
        compiler_params=pltpu.CompilerParams(vmem_limit_bytes=16 * 2**20),
    )(*(hold(v) for v in (acts, grads, G, At, dw, top)), hist_act, hist_weight, hist_grad)
    full = (1, M, R, F)
    return out_acts.reshape(full), out_grads.reshape(full), out_w[None], ha, hw, hg


def solution(mesh):
    placed = (P(None, "dp", "tensor"), P("pipe", None, "tensor"), P(None, "dp", "tensor"),
              P("pipe", None), P("pipe", None), P("pipe", None))
    return jax.shard_map(
        shards, mesh=mesh, in_specs=placed,
        out_specs=(P("pipe", None, "dp", "tensor"), P("pipe", None, "dp", "tensor"),
                   P("pipe", "dp", "tensor"), P("pipe", None), P("pipe", None), P("pipe", None)),
        check_vma=False)
```

```python
import functools

import jax
import jax.numpy as jnp
from jax import lax
from jax.experimental import pallas as pl
from jax.experimental.pallas import tpu as pltpu
from jax.sharding import PartitionSpec as P

MESH = pl.DeviceIdType.MESH
PARTS = 8
FIRST, LATER = (2, 3, 3), (4, 4)


def strides_below(index, count):
    low = (index & -index) if index else count
    step, found = low // 2, []
    while step:
        found.append(step)
        step //= 2
    return found


def low(i):
    return i & -i


def chunks_of(M, R):
    found = []
    for m in range(M):
        start = 0
        for part in FIRST if m == 0 else LATER:
            found.append((m, start, R * part // PARTS))
            start += R * part // PARTS
    return found


def units_of(M, R):
    return [(0, 0, R)] + [chunk for chunk in chunks_of(M, R) if chunk[0]]


def kernel(S, N, T, M, R, F, FA, chunks,
           acts, weights, cot, hist_a, hist_w, hist_g,
           xout, gout, G, At, dw, new_hist,
           w, wt, hv, cv, xin, xg, acc, gin, part, rs, A, pk, amax, gmax, gd, gh,
           w_sem, h_sem, in_sem, c_sem, x_ss, x_rs, ag_ss, ag_rs, g_ss, g_rs, rd_ss, rd_rs,
           G_ss, G_rs, Gr_ss, Gm_ss, A_ss, A_rs, B_ss, B_rs, p_ss, p_rs, hello, ready,
           gd_ss, gd_rs):
    s, d, t = lax.axis_index("pipe"), lax.axis_index("dp"), lax.axis_index("tensor")
    last = S - 1
    bf, f32 = jnp.bfloat16, jnp.float32
    NC = len(chunks)
    units = units_of(M, R)
    U = len(units)
    top = T // 2
    stages = []
    st = 1
    while st < T:
        stages.append(st)
        st *= 2

    def remote(src, dst, ss, rsem, **where):
        return pltpu.make_async_remote_copy(
            src_ref=src, dst_ref=dst, send_sem=ss, recv_sem=rsem,
            device_id=where, device_id_type=MESH)

    def signal(sem, **where):
        pl.semaphore_signal(sem, inc=1, device_id=where, device_id_type=MESH)

    barrier = pltpu.get_barrier_semaphore()
    for st in stages:
        signal(barrier, tensor=t ^ st)

    @pl.when(s > 0)
    def _():
        signal(barrier, pipe=s - 1)

    @pl.when(s < last)
    def _():
        signal(barrier, pipe=s + 1)

    @pl.when(d > 0)
    def _():
        signal(barrier, dp=d - 1)

    @pl.when(d < N - 1)
    def _():
        signal(barrier, dp=d + 1)

    def rows_at(c):
        m, start, n = chunks[c]
        return pl.ds(m * R + start, n)

    h_loads = [pltpu.make_async_copy(h, hv.at[i], h_sem)
               for i, h in enumerate((hist_a, hist_w, hist_g))]
    loads = [pltpu.make_async_copy(weights.at[b], w.at[b], w_sem.at[b]) for b in range(T)]
    first = chunks[0][2]
    in_loads = [pltpu.make_async_copy(acts.at[rows], xin.at[rows], in_sem.at[i])
                for i, rows in enumerate((pl.ds(0, first), pl.ds(first, M * R - first)))]
    cot_load = pltpu.make_async_copy(cot, cv, c_sem)
    for copy in h_loads:
        copy.start()

    @pl.when(s == 0)
    def _():
        for copy in in_loads:
            copy.start()

    pltpu.make_async_copy(hv, hv, h_sem).wait()
    for copy in loads:
        copy.start()

    @pl.when(s == last)
    def _():
        cot_load.start()

    def limit(i):
        return jnp.max(hv[i], axis=1, keepdims=True).astype(bf)

    lim_a, lim_w, lim_g = limit(0), limit(1), limit(2)

    def clip(v, lim):
        return jnp.minimum(jnp.maximum(v, -lim), lim)

    def fold(v):
        return jnp.max(jnp.abs(v).reshape(-1, 16, v.shape[-1]), axis=0)

    amax[...] = jnp.zeros_like(amax)
    gmax[...] = jnp.zeros_like(gmax)

    def enter():
        near = (s > 0).astype(jnp.int32) + (s < last).astype(jnp.int32)
        beside = (d > 0).astype(jnp.int32) + (d < N - 1).astype(jnp.int32)
        pl.semaphore_wait(barrier, len(stages) + near + beside)

    def greet(r):
        @pl.when(d > 0)
        def _():
            signal(hello.at[r, 0], dp=d - 1)

        @pl.when(d < N - 1)
        def _():
            signal(hello.at[r, 1], dp=d + 1)

    def greeted(r):
        @pl.when(d < N - 1)
        def _():
            pl.semaphore_wait(hello.at[r, 0], 1)

        @pl.when(d > 0)
        def _():
            pl.semaphore_wait(hello.at[r, 1], 1)

    up = jnp.minimum(s + 1, last)
    down = jnp.maximum(s - 1, 0)

    def gd_copy(c):
        return remote(part.at[top, rows_at(c)], gd.at[rows_at(c)], gd_ss, gd_rs.at[c], pipe=down, tensor=t ^ top)

    def x_copy(c):
        return remote(xout.at[rows_at(c)], xin.at[rows_at(c)], x_ss, x_rs.at[c], pipe=up)

    def g_copy(c):
        return remote(gh.at[rows_at(c)], gin.at[rows_at(c)], g_ss, g_rs.at[c], pipe=down)

    def ag_copy(c, j, st):
        i = j ^ st
        return remote(xg.at[j, rows_at(c)], xg.at[i, rows_at(c)], ag_ss, ag_rs.at[c, i - 1], tensor=t ^ st)

    def G_copy(c, origin, to, ss):
        m, start, n = chunks[c]
        rows = pl.ds(start, n)
        return remote(G.at[m, origin ^ d, rows], G.at[m, origin ^ to, rows], ss, G_rs.at[c, (origin ^ to) - 1], dp=to)

    def G_wait(c, origin):
        m, start, n = chunks[c]
        here = G.at[m, origin ^ d, pl.ds(start, n)]
        remote(here, here, G_ss.at[0], G_rs.at[c, (origin ^ d) - 1], dp=origin).wait_recv()

    def inside(at):
        return (at >= 0) & (at < N)

    def own_sends(act, mix=False):
        for i, step in enumerate((2, -2, 1, -1)):
            if abs(step) < N:
                here = inside(d + step)
                if mix and abs(step) == 2:
                    here = here & inside(d + step + step // 2)

                @pl.when(here)
                def _(i=i, to=d + step):
                    act(to, G_ss.at[i])

    def near_end(way):
        return inside(d - way) & inside(d + way) & ~inside(d + 2 * way)

    def relays(wait, act, mix=False):
        for i, way in enumerate((1, -1)):
            if mix:
                @pl.when(near_end(way))
                def _(i=i, way=way):
                    wait(d - way)
                    act(d - way, d + way, Gm_ss.at[i])

            for m in range(1, (N + 1) // 2):
                origin = d - way * 2 * m

                @pl.when(inside(origin) & inside(d + way))
                def _(i=i, way=way, m=m, origin=origin):
                    wait(origin)
                    for step in (1, 2):
                        if 2 * m + step < N:
                            @pl.when(inside(d + way * step))
                            def _(step=step):
                                act(origin, d + way * step, Gr_ss.at[i, m - 1, step - 1])

    ratio = N // T

    def in_block(r):
        start = lax.rem(r, ratio) * FA
        return t ^ lax.div(r, ratio), pl.ds(pl.multiple_of(start, FA), FA)

    piece = FA // T

    def cols_of(owner):
        return pl.ds(pl.multiple_of(owner * piece, piece), piece)

    def unit_of(c):
        return 0 if chunks[c][0] == 0 else units.index(chunks[c])

    def block(u, which, cols):
        m, start, n = units[u]
        return A.at[m, which, pl.ds(start, n), cols]

    def A_copy(c, k):
        m, start, n = chunks[c]
        r = d ^ k
        cols = pl.ds(pl.multiple_of(lax.rem(r, ratio) * FA + t * piece, piece), piece)
        return remote(xg.at[t ^ lax.div(r, ratio), rows_at(c), cols], A.at[m, k, pl.ds(start, n), cols_of(t)],
                      A_ss, A_rs.at[unit_of(c)], dp=r)

    def B_copy(u, j, st):
        i = j ^ st
        there = block(u, pl.ds(1, N - 1), cols_of(t ^ j))
        return remote(there, there, B_ss, B_rs.at[u, i - 1], tensor=t ^ st)

    def B_arrival(u, i):
        there = block(u, pl.ds(1, N - 1), cols_of(t ^ i))
        return remote(there, there, B_ss, B_rs.at[u, i - 1], tensor=t ^ low(i))

    def rd_copy(c, j, level):
        st = stages[level]
        i = j ^ st
        return remote(part.at[j, rows_at(c)], rs.at[level, i, rows_at(c)], rd_ss, rd_rs.at[c, i + st - 1],
                      tensor=t ^ st)

    def prep(c):
        rows = rows_at(c)

        @pl.when(s == 0)
        def _():
            if c < len(in_loads):
                in_loads[c].wait()

        @pl.when(s > 0)
        def _():
            x_copy(c).wait_recv()

        x = xin[rows]
        xg[0, rows] = clip(x, lim_a)
        for st in strides_below(0, T):
            ag_copy(c, 0, st).start()
        amax[...] = jnp.maximum(amax[...], fold(x))

    def clip_weights():
        peak = jnp.zeros((16, F), bf)
        for b in range(T):
            loads[b].wait()

            def body(i, m, b=b):
                rows = pl.ds(pl.multiple_of(i * 128, 128), 128)
                v = w[b, rows]
                w[b, rows] = clip(v, lim_w)
                return jnp.maximum(m, fold(v))

            peak = lax.fori_loop(0, F // 128, body, peak)
        return jnp.max(peak.astype(f32), keepdims=True).reshape(1, 1)

    def turn_weights(first, end):
        for b in range(first, end):
            def body(i, _, b=b):
                rows = pl.ds(pl.multiple_of(i * 128, 128), 128)
                wt[b, :, rows] = w[b, rows].T
                return 0

            lax.fori_loop(0, F // 128, body, 0)

    def fwd(c, between=None):
        rows = rows_at(c)
        n = chunks[c][2]

        def term(j):
            return jnp.dot(xg[j, rows], w[t ^ j], preferred_element_type=f32)

        for j in range(T):
            if j:
                ag_copy(c, j ^ low(j), low(j)).wait_recv()
                for st in strides_below(j, T):
                    ag_copy(c, j, st).start()
            if j == 0:
                if T == 1:
                    xout[rows] = (term(0) + xin[rows].astype(f32)).astype(bf)
            elif j == 1:
                y = term(0) + term(1)
                if T == 2:
                    xout[rows] = (y + xin[rows].astype(f32)).astype(bf)
                else:
                    acc[:n] = y
                    if between:
                        between()
            elif j < T - 1:
                acc[:n] += term(j)
            else:
                xout[rows] = (acc[:n] + term(j) + xin[rows].astype(f32)).astype(bf)

        if c == 0 and top:
            pl.semaphore_wait(ready, 1)

        @pl.when(s < last)
        def _():
            x_copy(c).start()

    def send_A(c):
        m, start, n = chunks[c]
        for k in range(1, N):
            A_copy(c, k).start()
        owner, cols = in_block(d)
        A[m, 0, pl.ds(start, n)] = xg[owner, rows_at(c), cols]

    def bwd(c, is_last):
        m, start, n = chunks[c]
        rows = rows_at(c)
        if is_last:
            gin[rows] = (cv[rows].astype(f32) * xout[rows].astype(f32)).astype(bf)
        else:
            g_copy(c).wait_recv()
            if top:
                gd_copy(c).wait_recv()
                gin[rows] = (gin[rows].astype(f32) + gd[rows].astype(f32)).astype(bf)
        g = gin[rows]
        G[m, 0, pl.ds(start, n)] = clip(g, lim_g)
        if c == NC - 1:
            gmax[...] = jnp.maximum(gmax[...], fold(g))
            send_peaks()
        send_G(c, is_last)
        if c < NC - 1:
            gmax[...] = jnp.maximum(gmax[...], fold(g))

        def settle(j):
            level = 0
            while not (j >> level) & 1:
                rd_copy(c, j ^ stages[level], level).wait_recv()
                part[j, rows] = (part[j, rows].astype(f32) + rs[level, j, rows].astype(f32)).astype(bf)
                level += 1
            rd_copy(c, j, level).start()
            if j == top:
                @pl.when(s > 0)
                def _():
                    gd_copy(c).start()

        def term(j):
            return jnp.dot(G[m, 0, pl.ds(start, n)], wt[t ^ j], preferred_element_type=f32).astype(bf)

        for j in reversed(range(1, T, 2)):
            y, z = term(j), term(j - 1)
            part[j, rows] = y
            part[j - 1, rows] = z
            rd_copy(c, j, 0).start()
            if j + 1 < T:
                settle(j + 1)
        if T == 1:
            part[0, rows] = term(0)

    def pass_on(c):
        rows = rows_at(c)

        @pl.when(s > 0)
        def _():
            total = gin[rows].astype(f32) + part[0, rows].astype(f32)
            for level in range(len(stages) - 1):
                rd_copy(c, stages[level], level).wait_recv()
                total = total + rs[level, 0, rows].astype(f32)
            gh[rows] = total.astype(bf)
            g_copy(c).start()

    def mixed(c, is_last):
        return is_last and M > 1 and 0 < c and chunks[c][0] == 0

    def send_G(c, is_last):
        own_sends(lambda to, ss: G_copy(c, d, to, ss).start(), mixed(c, is_last))

    def finb(c):
        rows = rows_at(c)
        total = gin[rows].astype(f32) + part[0, rows].astype(f32)
        for level in range(len(stages)):
            if level < len(stages) - 1:
                @pl.when(s == 0)
                def _(level=level):
                    rd_copy(c, stages[level], level).wait_recv()
            else:
                rd_copy(c, stages[level], level).wait_recv()
            total = total + rs[level, 0, rows].astype(f32)
        gout[rows] = total.astype(bf)

    def relay_G(c, is_last=False):
        relays(lambda origin: G_wait(c, origin), lambda origin, to, ss: G_copy(c, origin, to, ss).start(),
               mixed(c, is_last))

    def arrive_G(c, is_last=False):
        for step in range(1, N):
            for way in (1, -1):
                origin = d - way * step
                here = inside(origin)
                if step % 2 == 0:
                    here = here & ~inside(d + way)
                elif step == 1 and mixed(c, is_last):
                    here = here & ~near_end(way)

                @pl.when(here)
                def _(origin=origin):
                    G_wait(c, origin)

    def relay_A(u):
        there = block(u, pl.ds(1, N - 1), cols_of(t))
        remote(there, there, A_ss, A_rs.at[u], dp=d ^ 1).wait_recv()
        for st in strides_below(0, T):
            B_copy(u, 0, st).start()

    def relay_B(u):
        for j in range(1, T):
            if strides_below(j, T):
                B_arrival(u, j).wait_recv()
                for st in strides_below(j, T):
                    B_copy(u, j, st).start()

    def turn_A(u):
        m, start, n = units[u]
        group = max(1, 128 // n)
        for j in range(1, T):
            if not strides_below(j, T):
                B_arrival(u, j).wait_recv()
        for k in range(0, N, group):
            def body(i, _, k=k):
                cols = pl.ds(pl.multiple_of(i * 128, 128), 128)
                v = A[m, pl.ds(k, group), pl.ds(start, n), cols].reshape(group * n, 128)
                At[cols, pl.ds(N * (m * R + start) + k * n, group * n)] = v.T
                return 0

            lax.fori_loop(0, FA // 128, body, 0)

    def update(u):
        m, start, n = units[u]
        tile = min(256, FA)

        def body(i, _):
            rows = pl.ds(pl.multiple_of(i * tile, tile), tile)
            y = jnp.dot(At[rows, pl.ds(N * (m * R + start), N * n)], G[m, :, pl.ds(start, n)].reshape(N * n, F),
                        preferred_element_type=f32)
            if u == 0:
                dw[rows] = y
            else:
                dw[rows] += y
            return 0

        lax.fori_loop(0, FA // tile, body, 0)

    def peers():
        return [(k, j) for k in range(N) for j in range(T) if k or j]

    def p_copy(k, j):
        i = k * T + j
        return remote(pk.at[0], pk.at[i], p_ss, p_rs, dp=d ^ k, tensor=t ^ j)

    def send_peaks():
        row = lax.broadcasted_iota(jnp.int32, (8, 128), 0)
        top_a = jnp.max(amax[...].astype(f32), keepdims=True).reshape(1, 1)
        top_g = jnp.max(gmax[...].astype(f32), keepdims=True).reshape(1, 1)
        pk[0] = jnp.where(row == 0, top_a, jnp.where(row == 1, w_peak, top_g))
        for k, j in peers():
            p_copy(k, j).start()

    ends = [max(c for c in range(NC) if chunks[c][0] == m) for m in range(M)]

    def meet(first, end):
        for r in range(first, end):
            greeted(r)
            if r + 1 < N - 2:
                greet(r + 1)

    enter()
    greet(0)
    if top:
        signal(ready, tensor=t ^ top)

    @pl.when(s == 0)
    def _():
        prep(0)
        prep(1)

    w_peak = clip_weights()

    @pl.when(s > 0)
    def _():
        meet(0, 1)
        turn_weights(0, T)
        prep(0)
        meet(1, N - 2)

    def arrive(u, is_last=False):
        for c in range(NC):
            if unit_of(c) == u:
                arrive_G(c, is_last)

    @pl.when(s == last)
    def _():
        cot_load.wait()
        for c in range(NC):
            fwd(c, functools.partial(pass_on, c - 1) if c else functools.partial(prep, 1))
            send_A(c)
            bwd(c, True)
            if c + 2 < NC:
                prep(c + 2)
            if c == 1:
                relay_G(0, True)
            if c >= 3:
                relay_G(c - 2, True)
            if c >= 2:
                finb(c - 2)
        pass_on(NC - 1)
        for c in range(max(0, NC - 2), NC):
            finb(c)
        relay_G(NC - 2, True)
        for u in range(U):
            if 1 < u:
                turn_A(u - 2)
                relay_B(u - 1)
            relay_A(u)
            if u == 1:
                relay_B(0)
        if U > 1:
            turn_A(U - 2)
        for u in range(min(1, U - 1)):
            arrive(u, True)
            update(u)
        relay_B(U - 1)
        relay_G(NC - 1, True)
        turn_A(U - 1)
        for u in range(1, U - 1):
            arrive(u, True)
            update(u)

    @pl.when(s < last)
    def _():
        @pl.when(s > 0)
        def _():
            prep(1)

        spread = [0, 0] + [min(T, max(1, T - NC + c)) for c in range(2, NC)] + [T]
        for c in range(NC):
            fwd(c)
            if c + 2 < NC:
                prep(c + 2)
            if c < 2:
                @pl.when(s == 0)
                def _(c=c):
                    meet(max(0, N - 3) * c, N - 3 + c)
            if c:
                for b in range(0 if c == 1 else c, c + 1):
                    send_A(b)

                @pl.when(s == 0)
                def _(c=c):
                    turn_weights(spread[c], spread[c + 1])

        for c in range(NC + 3):
            if c == 0:
                relay_A(0)
            if c == NC:
                relay_G(NC - 1)
            if 1 <= c < NC:
                relay_G(c - 1)
            if c < NC:
                bwd(c, False)
                pass_on(c)
            if 1 <= c < U:
                relay_A(c)
            if 2 <= c < NC + 2:
                finb(c - 2)
            if 2 <= c < U + 2:
                relay_B(c - 2)
            if 3 <= c < U + 3:
                turn_A(c - 3)
        for u in range(U - 1):
            arrive(u)
            update(u)

    arrive(U - 1)

    def peakwait():
        there = pk.at[pl.ds(1, N * T - 1)]
        remote(there, there, p_ss, p_rs, dp=d ^ 1).wait_recv()
        peaks = jnp.max(pk[...], axis=0)
        for i in range(3):
            new_hist[i] = jnp.concatenate([peaks[i:i + 1, 0:1], hv[i][:, :-1]], axis=1)

    def sent(ref, sem):
        remote(ref, ref, sem, p_rs, dp=d ^ 1).wait_send()

    def finalwait():
        if top:
            sent(xg.at[pl.ds(0, T - 1)], ag_ss)
            sent(part.at[pl.ds(0, T - 1)], rd_ss)

            @pl.when(s > 0)
            def _():
                sent(gin, gd_ss)

        def own_sent(to, ss):
            sent(gin, ss)

        @pl.when(s < last)
        def _():
            own_sends(own_sent)

        @pl.when(s == last)
        def _():
            if M > 1:
                own_sends(lambda to, ss: sent(gin.at[pl.ds(0, R - first)], ss), True)
                own_sends(lambda to, ss: sent(gin.at[pl.ds(R - first, (M - 1) * R + first)], ss))
                for i, way in enumerate((1, -1)):
                    @pl.when(near_end(way))
                    def _(i=i):
                        sent(gin.at[pl.ds(0, R - first)], Gm_ss.at[i])
            else:
                own_sends(own_sent)

        relays(lambda origin: None, lambda origin, to, ss: sent(gin, ss))

        @pl.when(s < last)
        def _():
            sent(gin, x_ss)

        @pl.when(s > 0)
        def _():
            sent(gin, g_ss)

        sent(A.at[:, pl.ds(1, N - 1), :, cols_of(t)], A_ss)
        sent(A.at[:, pl.ds(1, N - 1), :, pl.ds(0, (T - 1) * piece)], B_ss)
        sent(pk.at[pl.ds(1, N * T - 1)], p_ss)

    peakwait()
    finalwait()


def finish(unit, lanes, tile, acts, grads, G, At, dw, new_hist,
           out_acts, out_grads, out_w, out_ha, out_hw, out_hg, held, sem, w_sem, h_sem):
    m, start, n = unit
    moves = [pltpu.make_async_copy(acts, out_acts, sem.at[0]),
             pltpu.make_async_copy(grads, out_grads, sem.at[1])]
    for i, out in enumerate((out_ha, out_hw, out_hg)):
        moves.append(pltpu.make_async_copy(new_hist.at[i], out, h_sem.at[i]))
    for copy in moves:
        copy.start()
    count, width = dw.shape[0] // tile, dw.shape[1]
    for i in range(count):
        rows = pl.ds(i * tile, tile)
        y = jnp.dot(At[rows, lanes], G[m, :, pl.ds(start, n)].reshape(-1, width), preferred_element_type=jnp.float32)
        if m:
            y = dw[rows] + y
        held[rows] = y.astype(held.dtype)
        moves.append(pltpu.make_async_copy(held.at[rows], out_w.at[rows], w_sem.at[i]))
        moves[-1].start()
    for copy in moves:
        copy.wait()


def shards(acts_in, weights, cotangent, hist_act, hist_weight, hist_grad):
    S, N, T = lax.axis_size("pipe"), lax.axis_size("dp"), lax.axis_size("tensor")
    M, R, F = acts_in.shape
    chunks = chunks_of(M, R)
    NC, RT = len(chunks), M * R
    FA = T * F // N
    bf, f32 = jnp.bfloat16, jnp.float32
    levels = max(1, T.bit_length() - 1)
    dma = pltpu.SemaphoreType.DMA
    hbm = pl.BlockSpec(memory_space=pltpu.HBM)
    vmem = pl.BlockSpec(memory_space=pltpu.VMEM)
    flat = (RT, F)
    H = hist_act.shape
    hist = jax.ShapeDtypeStruct(H, f32)
    half = max(1, (N + 1) // 2 - 1)
    units = units_of(M, R)
    unit = units[-1]
    acts, grads, G, At, dw, new_hist = pl.pallas_call(
        functools.partial(kernel, S, N, T, M, R, F, FA, chunks),
        out_shape=(pltpu.VMEM(flat, bf), pltpu.VMEM(flat, bf),
                   pltpu.VMEM((M, N, R, F), bf), pltpu.VMEM((FA, N * RT), bf),
                   pltpu.VMEM((FA, F), f32), pltpu.VMEM((3,) + H, f32)),
        in_specs=[hbm] * 6,
        out_specs=(vmem,) * 6,
        scratch_shapes=[
            pltpu.VMEM((T, F, F), bf),
            pltpu.VMEM((T, F, F), bf),
            pltpu.VMEM((3,) + H, f32),
            pltpu.VMEM(flat, bf),
            pltpu.VMEM(flat, bf),
            pltpu.VMEM((T,) + flat, bf),
            pltpu.VMEM((max(n for _, _, n in chunks), F), f32),
            pltpu.VMEM(flat, bf),
            pltpu.VMEM((T,) + flat, bf),
            pltpu.VMEM((levels, T) + flat, bf),
            pltpu.VMEM((M, N, R, FA), bf),
            pltpu.VMEM((N * T, 8, 128), f32),
            pltpu.VMEM((16, F), bf),
            pltpu.VMEM((16, F), bf),
            pltpu.VMEM(flat, bf),
            pltpu.VMEM(flat, bf),
            dma((T,)), dma(()), dma((2,)), dma(()), dma(()), dma((NC,)), dma(()), dma((NC, T - 1)),
            dma(()), dma((NC,)), dma(()), dma((NC, T - 1)),
            dma((4,)), dma((NC, N - 1)), dma((2, half, 2)), dma((2,)),
            dma(()), dma((len(units),)), dma(()), dma((len(units), T - 1)),
            dma(()), dma(()), pltpu.SemaphoreType.REGULAR((max(1, N - 2), 2)),
            pltpu.SemaphoreType.REGULAR, dma(()), dma((NC,)),
        ],
        compiler_params=pltpu.CompilerParams(
            collective_id=0, has_side_effects=True, vmem_limit_bytes=40 * 2**20),
    )(*(pltpu.with_memory_space_constraint(v, pltpu.HBM) for v in (
        acts_in.reshape(flat), weights.reshape(T, F, F), cotangent.reshape(flat),
        hist_act, hist_weight, hist_grad)))

    def hold(v):
        return pltpu.with_memory_space_constraint(v, pltpu.VMEM)

    tile = min(256, FA)
    out_acts, out_grads, out_w, ha, hw, hg = pl.pallas_call(
        functools.partial(finish, unit, pl.ds(N * (RT - unit[2]), N * unit[2]), tile),
        out_shape=(jax.ShapeDtypeStruct(flat, bf), jax.ShapeDtypeStruct(flat, bf),
                   jax.ShapeDtypeStruct((FA, F), bf), hist, hist, hist),
        in_specs=[vmem] * 6,
        out_specs=(hbm,) * 6,
        scratch_shapes=[pltpu.VMEM((FA, F), bf), dma((2,)), dma((FA // tile,)), dma((3,))],
        compiler_params=pltpu.CompilerParams(vmem_limit_bytes=16 * 2**20),
    )(*(hold(v) for v in (acts, grads, G, At, dw, new_hist)))
    full = (1, M, R, F)
    return out_acts.reshape(full), out_grads.reshape(full), out_w[None], ha, hw, hg


def solution(mesh):
    placed = (P(None, "dp", "tensor"), P("pipe", None, "tensor"), P(None, "dp", "tensor"),
              P("pipe", None), P("pipe", None), P("pipe", None))
    return jax.shard_map(
        shards, mesh=mesh, in_specs=placed,
        out_specs=(P("pipe", None, "dp", "tensor"), P("pipe", None, "dp", "tensor"),
                   P("pipe", "dp", "tensor"), P("pipe", None), P("pipe", None), P("pipe", None)),
        check_vma=False)
```
